128 devices in a mesh: wide: 8 (over z, x_hi), narrow: 4 (over y), depth: 4 (over x_lo, core).
Axes of the slice: x: 4 (x_hi: 2, x_lo: 2; x = x_hi * 2 + x_lo), y: 4, z: 4, core: 2. Of those that a mesh axis runs over, the one named last changes fastest.
Arguments:
- hidden_in: bfloat16 [2048, 4096], P(('wide', 'narrow'), 'depth'), may hold values from -36 to 36
- queries: bfloat16 [2048, 4096], P('wide', ('narrow', 'depth')), may hold values from -8 to 8
- lang_ids: int32 [2048], replicated, may hold values from 0 to 7
- owner_slot: int32 [8], replicated, may hold values from 0 to 7, each once
- enc_kv: bfloat16 [8, 2, 768, 4096], P('wide', None, None, ('narrow', 'depth')), may hold values from -7 to 7
- attn_proj: bfloat16 [4096, 4096], P(('narrow', 'depth')), may hold values from -0.09375 to 0.09375
- norm_gain: float32 [4096], replicated, may hold values from 0.25 to 1.75
- router_proj: float32 [4096, 4], replicated, may hold values from -0.09375 to 0.09375
- expert_ids: int32 [2048, 2], P('wide'), may hold values from 0 to 3, all different within a row; in each aligned block of 64 rows (0 to 63, 64 to 127, ...) at most 48 rows name the same one
- proj_in: bfloat16 [4, 4096, 5120], P('narrow', None, 'depth'), may hold values from -0.09375 to 0.09375
- proj_out: bfloat16 [4, 5120, 4096], P('narrow', 'depth'), may hold values from -0.078125 to 0.078125
Outputs:
- layer_out: bfloat16 [2048, 4096], P(('wide', 'narrow'), 'depth')
The draws below stay inside these ranges and needn't reach their ends.
Inputs may be any that keep to these rules, and one draw needn't show every extreme that they name: `owner_slot`: every slot once. `expert_ids`: each row names two different experts. Within each aligned block of 64 rows (the rows of one index of wide+narrow) no expert is named more than 48 times, a bound that some block reaches.
All inputs are finite; a program needn't handle non-finite values.
Results may differ from the reference program's by a relative error of at most 0.017.
Values may be sent and summed in bfloat16 or wider, within the bound.
A program may use at most 128 MiB of HBM per device.

```python
import math
import jax
import jax.numpy as jnp
import numpy as np
from jax import lax

D = 4096
HEADS = 64
HEAD_DIM = 64
FF = 5120
ENC = 768
TOK_DEV = 64
EXPERTS = 4
LANGS = 8
BATCH = 2048
CAP = 48


def draw_queries(key, part):
    base_draw = 1.5 * jax.random.truncated_normal(jax.random.fold_in(key, 1), -4.0, 4.0, (BATCH, HEADS * HEAD_DIM), jnp.float32)
    return base_draw.astype(jnp.bfloat16)


def draw_enc_kv(key, part):
    width_all = HEADS * HEAD_DIM
    offset = jax.random.truncated_normal(jax.random.fold_in(key, 2), -3.0, 3.0, (LANGS, 1, width_all), jnp.float32)
    noise_part = jax.random.truncated_normal(jax.random.fold_in(key, 3), -4.0, 4.0, (LANGS, ENC, width_all), jnp.float32)
    value_part = offset + noise_part
    key_part = jax.random.truncated_normal(jax.random.fold_in(key, 4), -4.0, 4.0, (LANGS, ENC, width_all), jnp.float32)
    return jnp.stack([key_part, value_part], axis=1).astype(jnp.bfloat16)


def draw_hidden_in(key, part):
    base_draw = jax.random.truncated_normal(jax.random.fold_in(key, 5), -4.0, 4.0, (BATCH, D), jnp.float32)
    return base_draw.astype(jnp.bfloat16)


def plant(drawn, key, least, largest):
    longest = drawn.shape.index(max(drawn.shape))
    spots = []
    for shift in (0, 1):
        where = [jax.random.randint(jax.random.fold_in(key, axis), (), 0, length) for axis, length in enumerate(drawn.shape)]
        where[longest] = (where[longest] + shift) % drawn.shape[longest]
        spots.append(tuple(where))
    return drawn.at[spots[0]].set(least).at[spots[1]].set(largest)


def shard_levels(key, shape, shards, least, largest):
    def one(dim, shards_of):
        draws = jax.random.uniform(jax.random.fold_in(jax.random.fold_in(key, 6), dim), (shards_of,), jnp.float32, least / len(shards), largest / len(shards))
        return jnp.repeat(jnp.exp(draws), shape[dim] // shards_of).reshape((-1,) + (1,) * (len(shape) - dim - 1))

    level = one(*shards[0])
    for cut in shards[1:]:
        level = level * one(*cut)
    return level


def cumulative_ranks(amount, skew):
    loads = [(1 << 20) // math.isqrt(standing ** skew) + 1 for standing in range(1, amount + 1)]
    deviation = 1 + sum(loads) // (1 << 30)
    return np.cumsum(np.array([max(1, weight // deviation) for weight in loads]))


def ranked(stream_key, dims, count, slope):
    grid = cumulative_ranks(count, slope)
    ticket = jax.random.randint(jax.random.fold_in(stream_key, 1), dims, 0, int(grid[count - 1]))
    grade = jnp.searchsorted(jnp.asarray(grid, jnp.int32), ticket, side="right")
    return jax.random.permutation(jax.random.fold_in(stream_key, 2), count)[grade].astype(jnp.int32)


def shared_out(key, own, number, rows, number_of, top, limit, lean):
    order = jax.random.permutation(key, number_of)
    heavy_load, ordinary = portions_of(number_of, rows * top, limit, lean, True), portions_of(number_of, rows * top, limit, lean, False)
    places = jnp.arange(number_of)

    def named(tallies, rotation):
        used = int((tallies > 0).sum())
        fixed = max(1, used // 4)
        moved = fixed + (places - fixed + rotation * (used - fixed)) % max(1, number_of - fixed)
        return jnp.zeros((number_of,), jnp.int32).at[order[jnp.where(places < fixed, places, moved)]].set(jnp.asarray(tallies, jnp.int32))

    tallies = jnp.where(number % 4 == 0, named(heavy_load, number // 4), named(ordinary, number - number // 4 - 1))
    mixed = jax.random.permutation(jax.random.fold_in(own, 3), number_of)
    source_of, receiver = mixed[0:number_of // 2 * 2:2], mixed[1:number_of // 2 * 2:2]
    margin = jnp.minimum(tallies[source_of] - 1, limit - tallies[receiver]) // 2
    margin = jnp.where((source_of == order[0]) | (receiver == order[0]) | (tallies[receiver] == 0), 0, jnp.maximum(margin, 0))
    moved = jax.random.randint(jax.random.fold_in(own, 4), (number_of // 2,), 0, 1 << 20) % (margin + 1)
    tallies = tallies.at[source_of].add(-moved).at[receiver].add(moved)
    items = jnp.searchsorted(jnp.cumsum(tallies), jnp.arange(rows * top), side="right").astype(jnp.int32)
    table = items.reshape(top, rows).T
    table = table[jax.random.permutation(jax.random.fold_in(own, 1), rows)]
    rotation = jax.random.randint(jax.random.fold_in(own, 2), (rows, 1), 0, top)
    return jnp.take_along_axis(table, (jnp.arange(top)[None, :] + rotation) % top, axis=1)


def portions_of(amount, total, most, slope, full):
    loads = [(1 << 20) // math.isqrt(grade ** slope) + 1 for grade in range(1, amount + 1)]
    largest = most if full else min(most, max(-(-total // amount), total * loads[0] // sum(loads)))
    least = 1 if total - largest >= amount - 1 else 0
    holding, spare = [largest] + [least] * (amount - 1), total - largest - least * (amount - 1)
    while spare > 0:
        free = [i for i in range(1, amount) if holding[i] < largest] or [i for i in range(1, amount) if holding[i] < most]
        whole, remaining = sum([loads[i] for i in free]), spare
        for i in free:
            more = min(most - holding[i], max(1, remaining * loads[i] // whole), spare)
            holding[i] = holding[i] + more
            spare = spare - more
    return np.array(holding)


def normal_values(key, shape, spread, reach, split=(), held_as=jnp.bfloat16):
    entries = spread * jax.random.normal(key, shape, jnp.float32)
    if split:
        entries = entries * shard_levels(key, shape, split, -0.22, 0.18)
    return jnp.clip(entries, -reach, reach).astype(held_as)


def setup_inputs(seed: int = 0) -> dict:
    streams_of = jax.random.split(jax.random.key(seed), 12)
    hidden_in = draw_hidden_in(jax.random.fold_in(streams_of[11], 71), 0)
    queries = draw_queries(jax.random.fold_in(streams_of[11], 71), 0)
    lang_ids = plant(ranked(streams_of[2], (BATCH,), LANGS, 2), jax.random.fold_in(streams_of[2], 3), 0, LANGS - 1).astype(jnp.int32)
    owner_slot = jax.random.permutation(streams_of[3], LANGS).astype(jnp.int32)
    enc_kv = draw_enc_kv(jax.random.fold_in(streams_of[11], 71), 0)
    attn_proj = normal_values(streams_of[5], (HEADS * HEAD_DIM, D), (HEADS * HEAD_DIM) ** -0.5, 0.09375, ((0, 16),))
    norm_gain = jnp.clip(1.0 + 0.15 * jax.random.normal(streams_of[6], (D,), jnp.float32), 0.25, 1.75)
    router_proj = normal_values(streams_of[7], (D, EXPERTS), D ** -0.5, 0.09375, (), jnp.float32)
    expert_ids_keys = jax.random.split(jax.random.fold_in(streams_of[8], 1), BATCH // TOK_DEV)
    expert_ids_turns = jax.random.permutation(jax.random.fold_in(streams_of[8], 3), BATCH // TOK_DEV)
    expert_ids = jax.vmap(lambda own, number: shared_out(jax.random.fold_in(streams_of[8], 2), own, number, TOK_DEV, EXPERTS, 2, CAP, 2))(expert_ids_keys, expert_ids_turns).reshape((BATCH, 2))
    proj_in = normal_values(streams_of[9], (EXPERTS, D, FF), D ** -0.5, 0.09375, ((0, 4), (2, 4)))
    proj_out = normal_values(streams_of[10], (EXPERTS, FF, D), FF ** -0.5, 0.078125, ((0, 4), (1, 4)))
    return {"hidden_in": hidden_in, "queries": queries, "lang_ids": lang_ids, "owner_slot": owner_slot, "enc_kv": enc_kv, "attn_proj": attn_proj, "norm_gain": norm_gain, "router_proj": router_proj, "expert_ids": expert_ids, "proj_in": proj_in, "proj_out": proj_out}


norm_eps = 1e-06

def reference(hidden_in, queries, lang_ids, owner_slot, enc_kv, attn_proj, norm_gain, router_proj, expert_ids, proj_in, proj_out):
    holder = owner_slot[lang_ids].astype(jnp.int32)
    block_rows = math.gcd(BATCH, 512)

    def attend(element):
        query_part, slot_tags = element
        query_rows = query_part.astype(jnp.float32).reshape(block_rows, HEADS, HEAD_DIM)

        def per_slot(running_sum, position):
            kv_pair = lax.dynamic_index_in_dim(enc_kv, position, 0, keepdims=False).astype(jnp.float32)
            key_rows = kv_pair[0].reshape(ENC, HEADS, HEAD_DIM)
            value_rows = kv_pair[1].reshape(ENC, HEADS, HEAD_DIM)
            scores = jnp.einsum('rhd,khd->rhk', query_rows, key_rows) * HEAD_DIM ** (-0.5)
            weights = jnp.exp(scores - lax.optimization_barrier(jnp.max(scores, axis=2, keepdims=True)))
            denominator = lax.optimization_barrier(jnp.sum(weights, axis=2))
            rounded = lax.optimization_barrier(weights.astype(jnp.bfloat16)).astype(jnp.float32)
            context = jnp.einsum('rhk,khd->rhd', rounded, value_rows) / denominator[:, :, None]
            return (running_sum + jnp.where((slot_tags == position)[:, None, None], context, 0.0), None)
        start_sum = jnp.zeros((block_rows, HEADS, HEAD_DIM), jnp.float32)
        running_sum, _ = lax.scan(per_slot, start_sum, jnp.arange(LANGS, dtype=jnp.int32))
        return running_sum.reshape(block_rows, HEADS * HEAD_DIM)
    context = lax.map(attend, (queries.reshape(BATCH // block_rows, block_rows, HEADS * HEAD_DIM), holder.reshape(BATCH // block_rows, block_rows)))
    context = context.reshape(BATCH, HEADS * HEAD_DIM).astype(jnp.bfloat16)
    attn_out = jnp.dot(context, attn_proj, preferred_element_type=jnp.float32)
    residual = (hidden_in.astype(jnp.float32) + attn_out).astype(jnp.bfloat16)
    resid_f32 = residual.astype(jnp.float32)
    inv_norm = lax.rsqrt(lax.optimization_barrier(jnp.mean(resid_f32 * resid_f32, axis=1)) + norm_eps)
    normed = (resid_f32 * inv_norm[:, None] * norm_gain[None, :]).astype(jnp.bfloat16)
    logits = jnp.dot(normed.astype(jnp.float32), router_proj, precision=lax.Precision.HIGHEST)
    pick_mask = expert_ids[:, :, None] == jnp.arange(EXPERTS, dtype=jnp.int32)[None, None, :]
    own_logit = lax.optimization_barrier(jnp.sum(jnp.where(pick_mask, logits[:, None, :], 0.0), axis=2))
    gates = jax.nn.sigmoid(own_logit - own_logit[:, ::-1])
    expert_weight = lax.optimization_barrier(jnp.sum(jnp.where(pick_mask, gates[:, :, None], 0.0), axis=1))

    def add_expert(running_sum, position):
        first_proj = lax.dynamic_index_in_dim(proj_in, position, 0, keepdims=False)
        second_proj = lax.dynamic_index_in_dim(proj_out, position, 0, keepdims=False)
        hidden_act = jnp.dot(normed, first_proj, preferred_element_type=jnp.float32)
        hidden_act = jax.nn.gelu(hidden_act, approximate=True).astype(jnp.bfloat16)
        expert_out = jnp.dot(hidden_act, second_proj, preferred_element_type=jnp.float32)
        expert_share = lax.optimization_barrier(jnp.sum(jnp.where(jnp.arange(EXPERTS, dtype=jnp.int32)[None, :] == position, expert_weight, 0.0), axis=1))
        return (running_sum + expert_share[:, None] * expert_out, None)
    start_total = jnp.zeros((BATCH, D), jnp.float32)
    moe_out, _ = lax.scan(add_expert, start_total, jnp.arange(EXPERTS, dtype=jnp.int32))
    return (resid_f32 + moe_out).astype(jnp.bfloat16)
```

```python
import math

import jax
import jax.numpy as jnp
from jax import lax
from jax.experimental import pallas as pl
from jax.experimental.pallas import tpu as pltpu
from jax.sharding import PartitionSpec as P

HEAD_DIM = 64
MESH = pl.DeviceIdType.MESH


neg_big = -1e30
norm_eps = 1e-06


def in_order(blocks, dim):
    shape = list(blocks.shape[1:])
    shape[dim] *= blocks.shape[0]
    return jnp.moveaxis(blocks, 0, dim).reshape(shape)


def sent_to_all(value, axis):
    peers = lax.axis_size(axis)
    return lax.all_to_all(
        jnp.broadcast_to(value[None], (peers, *value.shape)), axis, 0, 0, tiled=True
    )


def collect(value, axis, dim):
    return in_order(sent_to_all(value, axis), dim)


def in_blocks(value, dim, peers):
    before, after = (value.shape[:dim], value.shape[dim + 1 :])
    return jnp.moveaxis(value.reshape(*before, peers, -1, *after), dim, 0)


def sum_at_owner(value, axis, dim):
    blocks = in_blocks(value, dim, lax.axis_size(axis))
    arrived = lax.all_to_all(blocks, axis, split_axis=0, concat_axis=0, tiled=True)
    return arrived.astype(jnp.float32).sum(axis=0)


def empty_state(row_count, head_count):
    return (
        jnp.full((row_count, head_count), neg_big, jnp.float32),
        jnp.zeros((row_count, head_count), jnp.float32),
        jnp.zeros((row_count, head_count, HEAD_DIM), jnp.float32),
    )


def slot_update(running, query_rows, key_rows, value_rows, is_live):
    run_max, run_sum, run_acc = running
    scores = jnp.einsum(
        "rhd,khd->rhk", query_rows, key_rows, preferred_element_type=jnp.float32
    ) * HEAD_DIM ** (-0.5)
    new_max = jnp.where(is_live[:, None], jnp.maximum(run_max, jnp.max(scores, axis=2)), run_max)
    weights = jnp.where(is_live[:, None, None], jnp.exp(scores - new_max[:, :, None]), 0.0)
    shrink = jnp.exp(run_max - new_max)
    run_sum = run_sum * shrink + jnp.sum(weights, axis=2)
    taken_sum = jnp.einsum(
        "rhk,khd->rhd", weights.astype(jnp.bfloat16), value_rows, preferred_element_type=jnp.float32
    )
    return (new_max, run_sum, run_acc * shrink[:, :, None] + taken_sum)


def slot_scan(running, kv_block, first_slot, query_rows, slot_tags):
    head_count = query_rows.shape[1]

    def visit_slot(carried, element):
        kv_pair, position = element
        key_rows = kv_pair[0].reshape(kv_pair.shape[1], head_count, HEAD_DIM)
        value_rows = kv_pair[1].reshape(kv_pair.shape[1], head_count, HEAD_DIM)
        return (slot_update(carried, query_rows, key_rows, value_rows, slot_tags == position), None)

    positions = first_slot + jnp.arange(kv_block.shape[0], dtype=jnp.int32)
    running, _ = lax.scan(visit_slot, running, (kv_block, positions))
    return running


def finish(running):
    run_max, run_sum, run_acc = running
    safe_sum = jnp.where(run_sum > 0.0, run_sum, 1.0)
    return (run_acc / safe_sum[:, :, None]).reshape(run_acc.shape[0], -1)


def remote(src, dst, sems, slot, target):
    send_sems, recv_sems = sems
    return pltpu.make_async_remote_copy(
        src_ref=src,
        dst_ref=dst,
        send_sem=send_sems.at[slot],
        recv_sem=recv_sems.at[slot],
        device_id=target,
        device_id_type=MESH,
    )


def places():
    y, d = lax.axis_index("narrow"), lax.axis_index("depth")
    x_lo, core = d // 2, d % 2
    return {
        "y": y,
        "d": d,
        "x": x_lo,
        "core": core,
        "up": (y + 1) % 4,
        "down": (y + 3) % 4,
        "far": (y + 2) % 4,
        "mate_d": x_lo * 2 + (1 - core),
        "side_d": (1 - x_lo) * 2 + core,
        "mate_side_d": (1 - x_lo) * 2 + (1 - core),
        "to_mate": {"depth": x_lo * 2 + (1 - core)},
        "to_side": {"depth": (1 - x_lo) * 2 + core},
        "to_up": {"narrow": (y + 1) % 4},
        "to_down": {"narrow": (y + 3) % 4},
    }


def scatter_sum(at, sems, base, part, own, mate_out, mate_in, ring_out, ring_in, side_out, side_in, tile):
    rows_all, quarter = own.shape[1:]
    rows = rows_all // 4
    tiles = quarter // tile

    def rows_of(y):
        return pl.ds(pl.multiple_of(y * rows, rows), rows)

    def fill(target, which, column_block, cast):
        def one(t, _):
            col = pl.multiple_of(column_block * quarter + t * tile, tile)
            here = pl.ds(pl.multiple_of(t * tile, tile), tile)
            target[which, :, here] = cast(part(col))
            return 0

        lax.fori_loop(0, tiles, one, 0)

    bf16 = lambda v: v.astype(jnp.bfloat16)
    mates = [None, None]
    for which, column_block in ((1, at["mate_side_d"]), (0, at["mate_d"])):
        fill(mate_out, which, column_block, bf16)
        mates[which] = remote(mate_out.at[which], mate_in.at[which], sems, base + which, at["to_mate"])
        mates[which].start()
    for which, column_block in ((1, at["side_d"]), (0, at["d"])):
        fill(own, which, column_block, lambda v: v)

    def pair(which, y):
        return own[which, rows_of(y), :] + mate_in[which, rows_of(y), :].astype(jnp.float32)

    def send(slot, value, target):
        ring_out[slot] = bf16(value)
        copy = remote(ring_out.at[slot], ring_in.at[slot], sems, base + 2 + slot, target)
        copy.start()
        return copy

    mates[1].wait_recv()
    copies = [None] * 6
    copies[3] = send(3, pair(1, at["far"]), at["to_down"])
    mates[0].wait_recv()
    copies[0] = send(0, pair(0, at["far"]), at["to_up"])
    copies[1] = send(1, pair(1, at["up"]), at["to_up"])
    copies[4] = send(4, pair(0, at["down"]), at["to_down"])
    copies[3].wait_recv()
    copies[5] = send(5, pair(1, at["down"]) + ring_in[3].astype(jnp.float32), at["to_down"])
    copies[0].wait_recv()
    copies[2] = send(2, pair(0, at["up"]) + ring_in[0].astype(jnp.float32), at["to_up"])
    copies[1].wait_recv()
    copies[5].wait_recv()
    side_out[...] = bf16(pair(1, at["y"]) + ring_in[1].astype(jnp.float32) + ring_in[5].astype(jnp.float32))
    side = remote(side_out, side_in, sems, base + 8, at["to_side"])
    side.start()
    copies[4].wait_recv()
    copies[2].wait_recv()
    mine = pair(0, at["y"]) + ring_in[4].astype(jnp.float32) + ring_in[2].astype(jnp.float32)
    side.wait_recv()
    for copy in [*mates, *copies, side]:
        copy.wait_send()
    return mine + side_in[...].astype(jnp.float32)


def gather_all(at, sems, base, full):
    rows, quarter = full.shape[0] // 4, full.shape[1] // 4
    half = rows // 2

    def block(y, d, part=None):
        cols = pl.ds(pl.multiple_of(d * quarter, quarter), quarter)
        if part is None:
            return full.at[pl.ds(pl.multiple_of(y * rows, rows), rows), cols]
        return full.at[pl.ds(pl.multiple_of(y * rows + part * half, half), half), cols]

    sent = []

    def send(slot, y, d, target, part=None):
        ref = block(y, d, part)
        copy = remote(ref, ref, sems, base + slot, target)
        copy.start()
        sent.append(copy)

    def arrived(slot, y, d, part=None):
        ref = block(y, d, part)
        remote(ref, ref, sems, base + slot, at["to_mate"]).wait_recv()

    y, d, mate, side, mate_side = at["y"], at["d"], at["mate_d"], at["side_d"], at["mate_side_d"]
    up, down, far = at["up"], at["down"], at["far"]
    send(0, y, d, at["to_side"])
    send(1, y, d, at["to_up"])
    send(2, y, d, at["to_down"])
    send(3, y, d, at["to_mate"])
    arrived(0, y, side)
    send(4, y, side, at["to_up"])
    send(5, y, side, at["to_down"])
    send(6, y, side, at["to_mate"])
    arrived(1, down, d)
    send(7, down, d, at["to_up"], 0)
    send(8, down, d, at["to_mate"])
    arrived(2, up, d)
    send(9, up, d, at["to_down"], 1)
    send(10, up, d, at["to_mate"])
    arrived(4, down, side)
    send(11, down, side, at["to_up"], 0)
    send(12, down, side, at["to_mate"])
    arrived(5, up, side)
    send(13, up, side, at["to_down"], 1)
    send(14, up, side, at["to_mate"])
    arrived(7, far, d, 0)
    send(15, far, d, at["to_mate"], 0)
    arrived(9, far, d, 1)
    send(16, far, d, at["to_mate"], 1)
    arrived(11, far, side, 0)
    send(17, far, side, at["to_mate"], 0)
    arrived(13, far, side, 1)
    send(18, far, side, at["to_mate"], 1)
    arrived(3, y, mate)
    arrived(6, y, mate_side)
    arrived(8, down, mate)
    arrived(10, up, mate)
    arrived(12, down, mate_side)
    arrived(14, up, mate_side)
    arrived(15, far, mate, 0)
    arrived(16, far, mate, 1)
    arrived(17, far, mate_side, 0)
    arrived(18, far, mate_side, 1)
    for copy in sent:
        copy.wait_send()


def layer_kernel(
    context,
    hidden_in,
    norm_gain,
    router_parts,
    expert_ids,
    attn_proj_hbm,
    proj_in_hbm,
    proj_out_hbm,
    out,
    attn_proj,
    proj_in,
    proj_out,
    full,
    normed,
    act,
    gate,
    own,
    mate_out,
    mate_in,
    ring_out,
    ring_in,
    side_out,
    side_in,
    load_sems,
    send_sems,
    recv_sems,
):
    at = places()
    sems = (send_sems, recv_sems)
    loads = [
        pltpu.make_async_copy(attn_proj_hbm, attn_proj, load_sems.at[0]),
        pltpu.make_async_copy(proj_in_hbm.at[0], proj_in, load_sems.at[1]),
        pltpu.make_async_copy(proj_out_hbm.at[0], proj_out, load_sems.at[2]),
    ]
    for load in loads:
        load.start()
    barrier = pltpu.get_barrier_semaphore()
    for peer in ("to_mate", "to_side", "to_up", "to_down"):
        pl.semaphore_signal(barrier, inc=1, device_id=at[peer], device_id_type=MESH)
    pl.semaphore_wait(barrier, 4)

    rows, quarter = hidden_in.shape
    tile = min(512, quarter)

    def proj_part(col):
        return jnp.dot(
            context[...], attn_proj[:, pl.ds(col, tile)], preferred_element_type=jnp.float32
        )

    loads[0].wait()
    attn_out = scatter_sum(
        at, sems, 0, proj_part, own, mate_out.at[0], mate_in.at[0], ring_out.at[0], ring_in.at[0],
        side_out.at[0], side_in.at[0], tile,
    )
    my_rows = pl.ds(pl.multiple_of(at["y"] * rows, rows), rows)
    my_cols = pl.ds(pl.multiple_of(at["d"] * quarter, quarter), quarter)
    full[my_rows, my_cols] = (hidden_in[...].astype(jnp.float32) + attn_out).astype(jnp.bfloat16)
    gather_all(at, sems, 9, full)

    strip = 16

    def normalise(s, _):
        here = pl.ds(pl.multiple_of(s * strip, strip), strip)
        value = full[here, :].astype(jnp.float32)
        inv = lax.rsqrt(jnp.mean(value * value, axis=1, keepdims=True) + norm_eps)
        normed[here, :] = (value * inv * norm_gain[...]).astype(jnp.bfloat16)
        return 0

    lax.fori_loop(0, full.shape[0] // strip, normalise, 0)
    logit_parts = lax.dot_general(
        normed[...], router_parts[...], (((1,), (1,)), ((), ())), preferred_element_type=jnp.float32
    )
    ids = expert_ids[...]
    first, second = ids[:, 0:1], ids[:, 1:2]
    chosen = (first == at["y"]) | (second == at["y"])
    other = first + second - at["y"]
    lane = lax.broadcasted_iota(jnp.int32, logit_parts.shape, 1)
    expert_of = lane % 4
    signed = jnp.where(expert_of == at["y"], logit_parts, 0.0) - jnp.where(
        expert_of == other, logit_parts, 0.0
    )
    margin = jnp.sum(signed, axis=1, keepdims=True)
    gate[...] = jnp.where(chosen, 1.0 / (1.0 + jnp.exp(-margin)), 0.0)

    loads[1].wait()
    hidden = act.shape[1]
    step = 256 if hidden % 256 == 0 else hidden

    def first_layer(t, _):
        here = pl.ds(pl.multiple_of(t * step, step), step)
        value = jnp.dot(normed[...], proj_in[:, here], preferred_element_type=jnp.float32)
        act[:, here] = jax.nn.gelu(value, approximate=True).astype(jnp.bfloat16)
        return 0

    lax.fori_loop(0, hidden // step, first_layer, 0)
    loads[2].wait()

    def expert_part(col):
        return gate[...] * jnp.dot(
            act[...], proj_out[:, pl.ds(col, tile)], preferred_element_type=jnp.float32
        )

    combined = scatter_sum(
        at, sems, 28, expert_part, own, mate_out.at[1], mate_in.at[1], ring_out.at[1], ring_in.at[1],
        side_out.at[1], side_in.at[1], tile,
    )
    out[...] = (full[my_rows, my_cols].astype(jnp.float32) + combined).astype(jnp.bfloat16)


def layer_tail(context, hidden_in, norm_gain, router_proj, expert_ids, attn_proj, proj_in, proj_out):
    rows_all, inner = context.shape
    rows, quarter = hidden_in.shape
    width = attn_proj.shape[1]
    hidden = proj_in.shape[2]
    router_rows = router_proj.T
    high = lax.reduce_precision(router_rows, 8, 7)
    middle = lax.reduce_precision(router_rows - high, 8, 7)
    low = router_rows - high - middle
    router_parts = jnp.concatenate([high, middle, low, jnp.zeros_like(low)], axis=0).astype(jnp.bfloat16)
    vmem, hbm = pl.BlockSpec(memory_space=pltpu.VMEM), pl.BlockSpec(memory_space=pl.ANY)
    bf16 = jnp.bfloat16
    copies = 37
    return pl.pallas_call(
        layer_kernel,
        out_shape=jax.ShapeDtypeStruct((rows, quarter), bf16),
        in_specs=[vmem] * 5 + [hbm] * 3,
        out_specs=vmem,
        scratch_shapes=[
            pltpu.VMEM((inner, width), bf16),
            pltpu.VMEM((width, hidden), bf16),
            pltpu.VMEM((hidden, width), bf16),
            pltpu.VMEM((rows_all, width), bf16),
            pltpu.VMEM((rows_all, width), bf16),
            pltpu.VMEM((rows_all, hidden), bf16),
            pltpu.VMEM((rows_all, 1), jnp.float32),
            pltpu.VMEM((2, rows_all, quarter), jnp.float32),
            pltpu.VMEM((2, 2, rows_all, quarter), bf16),
            pltpu.VMEM((2, 2, rows_all, quarter), bf16),
            pltpu.VMEM((2, 6, rows, quarter), bf16),
            pltpu.VMEM((2, 6, rows, quarter), bf16),
            pltpu.VMEM((2, rows, quarter), bf16),
            pltpu.VMEM((2, rows, quarter), bf16),
            pltpu.SemaphoreType.DMA((3,)),
            pltpu.SemaphoreType.DMA((copies,)),
            pltpu.SemaphoreType.DMA((copies,)),
        ],
        compiler_params=pltpu.CompilerParams(
            collective_id=0, has_side_effects=True, vmem_limit_bytes=60 * 1024 * 1024
        ),
        name="layer_tail",
    )(context, hidden_in, norm_gain.reshape(1, -1), router_parts, expert_ids, attn_proj, proj_in, proj_out)


def shards(
    hidden_in,
    queries,
    lang_ids,
    owner_slot,
    enc_kv,
    attn_proj,
    norm_gain,
    router_proj,
    expert_ids,
    proj_in,
    proj_out,
):
    head_count = queries.shape[1] // HEAD_DIM
    lang_count = owner_slot.shape[0]
    lang_match = lang_ids[:, None] == jnp.arange(lang_count, dtype=jnp.int32)[None, :]
    holder = jnp.sum(jnp.where(lang_match, owner_slot[None, :], 0), axis=1)
    first_slot = lax.axis_index("wide") * enc_kv.shape[0]
    segment = collect(queries, "wide", 0)
    row_count = segment.shape[0]
    block_rows = math.gcd(row_count, 512)

    def one_block(element):
        part_rows, part_tags = element
        running = slot_scan(
            empty_state(block_rows, head_count),
            enc_kv,
            first_slot,
            part_rows.reshape(block_rows, head_count, HEAD_DIM),
            part_tags,
        )
        return finish(running)

    blocks_out = lax.map(
        one_block,
        (
            segment.reshape(row_count // block_rows, block_rows, segment.shape[1]),
            holder.reshape(row_count // block_rows, block_rows),
        ),
    )
    partial_context = blocks_out.reshape(row_count, segment.shape[1])
    context = sum_at_owner(partial_context.astype(jnp.bfloat16), "wide", 0).astype(jnp.bfloat16)
    return layer_tail(
        context, hidden_in, norm_gain, router_proj, expert_ids, attn_proj, proj_in, proj_out
    )


def solution(mesh):
    return jax.shard_map(
        shards,
        mesh=mesh,
        in_specs=(
            P(("wide", "narrow"), "depth"),
            P("wide", ("narrow", "depth")),
            P(),
            P(),
            P("wide", None, None, ("narrow", "depth")),
            P(("narrow", "depth"), None),
            P(),
            P(),
            P("wide", None),
            P("narrow", None, "depth"),
            P("narrow", "depth", None),
        ),
        out_specs=P(("wide", "narrow"), "depth"),
        check_vma=False,
    )
```

```python
import math

import jax
import jax.numpy as jnp
from jax import lax
from jax.experimental import pallas as pl
from jax.experimental.pallas import tpu as pltpu
from jax.sharding import PartitionSpec as P

HEAD_DIM = 64
MESH = pl.DeviceIdType.MESH


norm_eps = 1e-06


def remote(src, dst, sems, slot, target):
    send_sems, recv_sems = sems
    return pltpu.make_async_remote_copy(
        src_ref=src,
        dst_ref=dst,
        send_sem=send_sems.at[slot],
        recv_sem=recv_sems.at[slot],
        device_id=target,
        device_id_type=MESH,
    )


def places():
    y, d = lax.axis_index("narrow"), lax.axis_index("depth")
    x_lo, core = d // 2, d % 2
    return {
        "y": y,
        "d": d,
        "x": x_lo,
        "core": core,
        "up": (y + 1) % 4,
        "down": (y + 3) % 4,
        "far": (y + 2) % 4,
        "mate_d": x_lo * 2 + (1 - core),
        "side_d": (1 - x_lo) * 2 + core,
        "mate_side_d": (1 - x_lo) * 2 + (1 - core),
        "to_mate": {"depth": x_lo * 2 + (1 - core)},
        "to_side": {"depth": (1 - x_lo) * 2 + core},
        "to_up": {"narrow": (y + 1) % 4},
        "to_down": {"narrow": (y + 3) % 4},
    }


def scatter_sum(at, sems, base, part, own, mate_out, mate_in, ring_out, ring_in, side_out, side_in, tile):
    rows_all, quarter = own.shape[1:]
    rows = rows_all // 4
    tiles = quarter // tile

    def rows_of(y):
        return pl.ds(pl.multiple_of(y * rows, rows), rows)

    def fill(target, which, column_block, cast):
        def one(t, _):
            col = pl.multiple_of(column_block * quarter + t * tile, tile)
            here = pl.ds(pl.multiple_of(t * tile, tile), tile)
            target[which, :, here] = cast(part(col))
            return 0

        lax.fori_loop(0, tiles, one, 0)

    bf16 = lambda v: v.astype(jnp.bfloat16)
    mates = [None, None]
    for which, column_block in ((1, at["mate_side_d"]), (0, at["mate_d"])):
        fill(mate_out, which, column_block, bf16)
        mates[which] = remote(mate_out.at[which], mate_in.at[which], sems, base + which, at["to_mate"])
        mates[which].start()
    for which, column_block in ((1, at["side_d"]), (0, at["d"])):
        fill(own, which, column_block, lambda v: v)

    def pair(which, y):
        return own[which, rows_of(y), :] + mate_in[which, rows_of(y), :].astype(jnp.float32)

    def send(slot, value, target):
        ring_out[slot] = bf16(value)
        copy = remote(ring_out.at[slot], ring_in.at[slot], sems, base + 2 + slot, target)
        copy.start()
        return copy

    mates[1].wait_recv()
    copies = [None] * 6
    copies[3] = send(3, pair(1, at["far"]), at["to_down"])
    mates[0].wait_recv()
    copies[0] = send(0, pair(0, at["far"]), at["to_up"])
    copies[1] = send(1, pair(1, at["up"]), at["to_up"])
    copies[4] = send(4, pair(0, at["down"]), at["to_down"])
    copies[3].wait_recv()
    copies[5] = send(5, pair(1, at["down"]) + ring_in[3].astype(jnp.float32), at["to_down"])
    copies[0].wait_recv()
    copies[2] = send(2, pair(0, at["up"]) + ring_in[0].astype(jnp.float32), at["to_up"])
    copies[1].wait_recv()
    copies[5].wait_recv()
    side_out[...] = bf16(pair(1, at["y"]) + ring_in[1].astype(jnp.float32) + ring_in[5].astype(jnp.float32))
    side = remote(side_out, side_in, sems, base + 8, at["to_side"])
    side.start()
    copies[4].wait_recv()
    copies[2].wait_recv()
    mine = pair(0, at["y"]) + ring_in[4].astype(jnp.float32) + ring_in[2].astype(jnp.float32)
    side.wait_recv()
    for copy in [*mates, *copies, side]:
        copy.wait_send()
    return mine + side_in[...].astype(jnp.float32)


def gather_all(at, sems, base, full):
    rows, quarter = full.shape[0] // 4, full.shape[1] // 4
    half = rows // 2

    def block(y, d, part=None):
        cols = pl.ds(pl.multiple_of(d * quarter, quarter), quarter)
        if part is None:
            return full.at[pl.ds(pl.multiple_of(y * rows, rows), rows), cols]
        return full.at[pl.ds(pl.multiple_of(y * rows + part * half, half), half), cols]

    sent = []

    def send(slot, y, d, target, part=None):
        ref = block(y, d, part)
        copy = remote(ref, ref, sems, base + slot, target)
        copy.start()
        sent.append(copy)

    def arrived(slot, y, d, part=None):
        ref = block(y, d, part)
        remote(ref, ref, sems, base + slot, at["to_mate"]).wait_recv()

    y, d, mate, side, mate_side = at["y"], at["d"], at["mate_d"], at["side_d"], at["mate_side_d"]
    up, down, far = at["up"], at["down"], at["far"]
    send(0, y, d, at["to_side"])
    send(1, y, d, at["to_up"])
    send(2, y, d, at["to_down"])
    send(3, y, d, at["to_mate"])
    arrived(0, y, side)
    send(4, y, side, at["to_up"])
    send(5, y, side, at["to_down"])
    send(6, y, side, at["to_mate"])
    arrived(1, down, d)
    send(7, down, d, at["to_up"], 0)
    send(8, down, d, at["to_mate"])
    arrived(2, up, d)
    send(9, up, d, at["to_down"], 1)
    send(10, up, d, at["to_mate"])
    arrived(4, down, side)
    send(11, down, side, at["to_up"], 0)
    send(12, down, side, at["to_mate"])
    arrived(5, up, side)
    send(13, up, side, at["to_down"], 1)
    send(14, up, side, at["to_mate"])
    arrived(7, far, d, 0)
    send(15, far, d, at["to_mate"], 0)
    arrived(9, far, d, 1)
    send(16, far, d, at["to_mate"], 1)
    arrived(11, far, side, 0)
    send(17, far, side, at["to_mate"], 0)
    arrived(13, far, side, 1)
    send(18, far, side, at["to_mate"], 1)
    arrived(3, y, mate)
    arrived(6, y, mate_side)
    arrived(8, down, mate)
    arrived(10, up, mate)
    arrived(12, down, mate_side)
    arrived(14, up, mate_side)
    arrived(15, far, mate, 0)
    arrived(16, far, mate, 1)
    arrived(17, far, mate_side, 0)
    arrived(18, far, mate_side, 1)
    for copy in sent:
        copy.wait_send()


def wide_places():
    w = lax.axis_index("wide")
    z, x = w // 2, w % 2
    up, down, far = (z + 1) % 4, (z + 3) % 4, (z + 2) % 4
    order = [z * 2 + x, up * 2 + x, down * 2 + x, z * 2 + 1 - x, far * 2 + x, up * 2 + 1 - x, down * 2 + 1 - x, far * 2 + 1 - x]
    return {"w": w, "order": order}


OWN, UP, DOWN, SIDE, FAR, UP_SIDE, DOWN_SIDE, FAR_SIDE = range(8)
BACK = (OWN, DOWN, UP, SIDE, FAR, DOWN_SIDE, UP_SIDE, FAR_SIDE)


def attend(at, sems, base, lang_rows, owner_slot, asked, keys, values, marks, answer, returned, context):
    rows, feats = context.shape
    heads = feats // HEAD_DIM
    length = keys.shape[2]
    half = rows // 2
    order = at["order"]

    def send(slot, src_slot, dst_slot, target_slot, part=None):
        src, dst = asked.at[src_slot], asked.at[dst_slot]
        if part is not None:
            here = pl.ds(part * half, half)
            src, dst = asked.at[src_slot, here], asked.at[dst_slot, here]
        remote(src, dst, sems, base + slot, {"wide": order[target_slot]}).start()

    def arrived(slot, dst_slot, part=None):
        dst = asked.at[dst_slot] if part is None else asked.at[dst_slot, pl.ds(part * half, half)]
        remote(dst, dst, sems, base + slot, {"wide": order[SIDE]}).wait_recv()

    send(0, OWN, SIDE, SIDE)
    send(1, OWN, DOWN, UP)
    send(2, OWN, UP, DOWN)

    group = jnp.int32(0)
    for g in range(owner_slot.shape[0]):
        group = group + jnp.where(owner_slot[g] == at["w"], g, 0)
    marks[...] = jnp.where(lang_rows[...] == group, 1.0, 0.0).T
    scale = HEAD_DIM ** (-0.5) * math.log2(math.e)

    def one_block(k, _):
        @pl.when(k == UP)
        def _():
            arrived(1, DOWN)
            send(3, DOWN, FAR, UP, 0)
            arrived(2, UP)
            send(4, UP, FAR, DOWN, 1)

        @pl.when(k == DOWN)
        def _():
            arrived(0, SIDE)
            send(5, SIDE, DOWN_SIDE, UP)
            send(6, SIDE, UP_SIDE, DOWN)

        @pl.when(k == FAR)
        def _():
            arrived(3, FAR, 0)
            arrived(4, FAR, 1)
            arrived(5, DOWN_SIDE)
            send(7, DOWN_SIDE, FAR_SIDE, UP, 0)
            arrived(6, UP_SIDE)
            send(8, UP_SIDE, FAR_SIDE, DOWN, 1)

        @pl.when(k == FAR_SIDE)
        def _():
            arrived(7, FAR_SIDE, 0)
            arrived(8, FAR_SIDE, 1)

        source = jnp.int32(0)
        for slot in range(8):
            source = source + jnp.where(k == slot, order[slot], 0)
        lane = lax.broadcasted_iota(jnp.int32, marks.shape, 1)
        here = jnp.sum(jnp.where(lane == source, marks[...], 0.0), axis=1, keepdims=True)
        query = asked[k]
        total = jnp.zeros((rows, feats), jnp.float32)
        for head in range(heads):
            scores = jnp.dot(query, keys[head], preferred_element_type=jnp.float32)
            top = jnp.max(scores, axis=1, keepdims=True)
            weights = jnp.exp2((scores - top) * scale)
            below = jnp.sum(weights, axis=1, keepdims=True)
            taken = jnp.dot(weights.astype(jnp.bfloat16), values[head], preferred_element_type=jnp.float32)
            total = total + taken * (here / below)
        answer[k] = total.astype(jnp.bfloat16)
        for slot in range(1, 8):

            @pl.when(k == slot)
            def _():
                remote(
                    answer.at[slot], returned.at[BACK[slot]], sems, base + 8 + slot, {"wide": order[slot]}
                ).start()

        return 0

    lax.fori_loop(0, 8, one_block, 0)
    summed = answer[OWN].astype(jnp.float32)
    for slot in range(1, 8):
        remote(answer.at[slot], returned.at[BACK[slot]], sems, base + 8 + slot, {"wide": order[slot]}).wait_recv()
    for slot in range(1, 8):
        summed = summed + returned[slot].astype(jnp.float32)
    context[...] = summed.astype(jnp.bfloat16)
    for slot in range(9):
        part = slot in (3, 4, 7, 8)
        src = asked.at[OWN, pl.ds(0, half)] if part else asked.at[OWN]
        remote(src, src, sems, base + slot, {"wide": order[SIDE]}).wait_send()
    for slot in range(1, 8):
        remote(answer.at[slot], returned.at[BACK[slot]], sems, base + 8 + slot, {"wide": order[slot]}).wait_send()


def spread_heads(kv, keys, values):
    heads = keys.shape[0]
    flipped = kv[0].T
    plain = kv[1]
    for head in range(heads):
        place = lax.broadcasted_iota(jnp.int32, flipped.shape, 0) // HEAD_DIM
        keys[head] = jnp.where(place == head, flipped, jnp.zeros_like(flipped))
        place = lax.broadcasted_iota(jnp.int32, plain.shape, 1) // HEAD_DIM
        values[head] = jnp.where(place == head, plain, jnp.zeros_like(plain))


def layer_kernel(
    owner_slot,
    lang_rows,
    hidden_in,
    norm_gain,
    router_parts,
    expert_ids,
    queries_hbm,
    enc_kv_hbm,
    attn_proj_hbm,
    proj_in_hbm,
    proj_out_hbm,
    out,
    asked,
    kv,
    keys,
    values,
    marks,
    answer,
    returned,
    context,
    attn_proj,
    proj_in,
    proj_out,
    full,
    normed,
    act,
    gate,
    own,
    mate_out,
    mate_in,
    ring_out,
    ring_in,
    side_out,
    side_in,
    load_sems,
    send_sems,
    recv_sems,
):
    at = places()
    sems = (send_sems, recv_sems)
    wide_at = wide_places()
    query_load = pltpu.make_async_copy(queries_hbm, asked.at[OWN], load_sems.at[3])
    query_load.start()
    kv_load = pltpu.make_async_copy(enc_kv_hbm.at[0], kv, load_sems.at[4])
    kv_load.start()
    loads = [
        pltpu.make_async_copy(attn_proj_hbm, attn_proj, load_sems.at[0]),
        pltpu.make_async_copy(proj_in_hbm.at[0], proj_in, load_sems.at[1]),
        pltpu.make_async_copy(proj_out_hbm.at[0], proj_out, load_sems.at[2]),
    ]
    for load in loads:
        load.start()
    barrier = pltpu.get_barrier_semaphore()
    for peer in ("to_mate", "to_side", "to_up", "to_down"):
        pl.semaphore_signal(barrier, inc=1, device_id=at[peer], device_id_type=MESH)
    for slot in range(1, 8):
        peer = {"wide": wide_at["order"][slot]}
        pl.semaphore_signal(barrier, inc=1, device_id=peer, device_id_type=MESH)
    kv_load.wait()
    spread_heads(kv, keys, values)
    query_load.wait()
    pl.semaphore_wait(barrier, 11)
    attend(
        wide_at, sems, 37, lang_rows, owner_slot, asked, keys, values, marks, answer, returned, context
    )

    rows, quarter = hidden_in.shape
    tile = min(512, quarter)

    def proj_part(col):
        return jnp.dot(
            context[...], attn_proj[:, pl.ds(col, tile)], preferred_element_type=jnp.float32
        )

    loads[0].wait()
    attn_out = scatter_sum(
        at, sems, 0, proj_part, own, mate_out.at[0], mate_in.at[0], ring_out.at[0], ring_in.at[0],
        side_out.at[0], side_in.at[0], tile,
    )
    my_rows = pl.ds(pl.multiple_of(at["y"] * rows, rows), rows)
    my_cols = pl.ds(pl.multiple_of(at["d"] * quarter, quarter), quarter)
    full[my_rows, my_cols] = (hidden_in[...].astype(jnp.float32) + attn_out).astype(jnp.bfloat16)
    gather_all(at, sems, 9, full)

    strip = 16

    def normalise(s, _):
        here = pl.ds(pl.multiple_of(s * strip, strip), strip)
        value = full[here, :].astype(jnp.float32)
        inv = lax.rsqrt(jnp.mean(value * value, axis=1, keepdims=True) + norm_eps)
        normed[here, :] = (value * inv * norm_gain[...]).astype(jnp.bfloat16)
        return 0

    lax.fori_loop(0, full.shape[0] // strip, normalise, 0)
    logit_parts = lax.dot_general(
        normed[...], router_parts[...], (((1,), (1,)), ((), ())), preferred_element_type=jnp.float32
    )
    ids = expert_ids[...]
    first, second = ids[:, 0:1], ids[:, 1:2]
    chosen = (first == at["y"]) | (second == at["y"])
    other = first + second - at["y"]
    lane = lax.broadcasted_iota(jnp.int32, logit_parts.shape, 1)
    expert_of = lane % 4
    signed = jnp.where(expert_of == at["y"], logit_parts, 0.0) - jnp.where(
        expert_of == other, logit_parts, 0.0
    )
    margin = jnp.sum(signed, axis=1, keepdims=True)
    gate[...] = jnp.where(chosen, 1.0 / (1.0 + jnp.exp(-margin)), 0.0)

    loads[1].wait()
    hidden = act.shape[1]
    step = 256 if hidden % 256 == 0 else hidden

    def first_layer(t, _):
        here = pl.ds(pl.multiple_of(t * step, step), step)
        value = jnp.dot(normed[...], proj_in[:, here], preferred_element_type=jnp.float32)
        act[:, here] = jax.nn.gelu(value, approximate=True).astype(jnp.bfloat16)
        return 0

    lax.fori_loop(0, hidden // step, first_layer, 0)
    loads[2].wait()

    def expert_part(col):
        return gate[...] * jnp.dot(
            act[...], proj_out[:, pl.ds(col, tile)], preferred_element_type=jnp.float32
        )

    combined = scatter_sum(
        at, sems, 28, expert_part, own, mate_out.at[1], mate_in.at[1], ring_out.at[1], ring_in.at[1],
        side_out.at[1], side_in.at[1], tile,
    )
    out[...] = (full[my_rows, my_cols].astype(jnp.float32) + combined).astype(jnp.bfloat16)


def layer_step(
    hidden_in,
    queries,
    lang_ids,
    owner_slot,
    enc_kv,
    attn_proj,
    norm_gain,
    router_proj,
    expert_ids,
    proj_in,
    proj_out,
):
    rows_all, inner = queries.shape
    rows, quarter = hidden_in.shape
    width = attn_proj.shape[1]
    hidden = proj_in.shape[2]
    length = enc_kv.shape[2]
    heads = inner // HEAD_DIM
    router_rows = router_proj.T
    high = lax.reduce_precision(router_rows, 8, 7)
    middle = lax.reduce_precision(router_rows - high, 8, 7)
    low = router_rows - high - middle
    router_parts = jnp.concatenate([high, middle, low, jnp.zeros_like(low)], axis=0).astype(jnp.bfloat16)
    vmem, hbm = pl.BlockSpec(memory_space=pltpu.VMEM), pl.BlockSpec(memory_space=pl.ANY)
    bf16 = jnp.bfloat16
    copies = 37 + 16
    return pl.pallas_call(
        layer_kernel,
        out_shape=jax.ShapeDtypeStruct((rows, quarter), bf16),
        in_specs=[pl.BlockSpec(memory_space=pltpu.SMEM)] + [vmem] * 5 + [hbm] * 5,
        out_specs=vmem,
        scratch_shapes=[
            pltpu.VMEM((8, rows_all, inner), bf16),
            pltpu.VMEM((2, length, inner), bf16),
            pltpu.VMEM((heads, inner, length), bf16),
            pltpu.VMEM((heads, length, inner), bf16),
            pltpu.VMEM((rows_all, 8), jnp.float32),
            pltpu.VMEM((8, rows_all, inner), bf16),
            pltpu.VMEM((8, rows_all, inner), bf16),
            pltpu.VMEM((rows_all, inner), bf16),
            pltpu.VMEM((inner, width), bf16),
            pltpu.VMEM((width, hidden), bf16),
            pltpu.VMEM((hidden, width), bf16),
            pltpu.VMEM((rows_all, width), bf16),
            pltpu.VMEM((rows_all, width), bf16),
            pltpu.VMEM((rows_all, hidden), bf16),
            pltpu.VMEM((rows_all, 1), jnp.float32),
            pltpu.VMEM((2, rows_all, quarter), jnp.float32),
            pltpu.VMEM((2, 2, rows_all, quarter), bf16),
            pltpu.VMEM((2, 2, rows_all, quarter), bf16),
            pltpu.VMEM((2, 6, rows, quarter), bf16),
            pltpu.VMEM((2, 6, rows, quarter), bf16),
            pltpu.VMEM((2, rows, quarter), bf16),
            pltpu.VMEM((2, rows, quarter), bf16),
            pltpu.SemaphoreType.DMA((5,)),
            pltpu.SemaphoreType.DMA((copies,)),
            pltpu.SemaphoreType.DMA((copies,)),
        ],
        compiler_params=pltpu.CompilerParams(
            collective_id=0, has_side_effects=True, vmem_limit_bytes=60 * 1024 * 1024
        ),
        name="layer_step",
    )(
        owner_slot,
        lang_ids.reshape(8, rows_all),
        hidden_in,
        norm_gain.reshape(1, -1),
        router_parts,
        expert_ids,
        queries,
        enc_kv,
        attn_proj,
        proj_in,
        proj_out,
    )


def solution(mesh):
    return jax.shard_map(
        layer_step,
        mesh=mesh,
        in_specs=(
            P(("wide", "narrow"), "depth"),
            P("wide", ("narrow", "depth")),
            P(),
            P(),
            P("wide", None, None, ("narrow", "depth")),
            P(("narrow", "depth"), None),
            P(),
            P(),
            P("wide", None),
            P("narrow", None, "depth"),
            P("narrow", "depth", None),
        ),
        out_specs=P(("wide", "narrow"), "depth"),
        check_vma=False,
    )
```

```python
import math

import jax
import jax.numpy as jnp
from jax import lax
from jax.experimental import pallas as pl
from jax.experimental.pallas import tpu as pltpu
from jax.sharding import PartitionSpec as P

HEAD_DIM = 64
MESH = pl.DeviceIdType.MESH


norm_eps = 1e-06


def remote(src, dst, sems, slot, target):
    send_sems, recv_sems = sems
    return pltpu.make_async_remote_copy(
        src_ref=src,
        dst_ref=dst,
        send_sem=send_sems.at[slot],
        recv_sem=recv_sems.at[slot],
        device_id=target,
        device_id_type=MESH,
    )


def places():
    y, d = lax.axis_index("narrow"), lax.axis_index("depth")
    x_lo, core = d // 2, d % 2
    return {
        "y": y,
        "d": d,
        "x": x_lo,
        "core": core,
        "up": (y + 1) % 4,
        "down": (y + 3) % 4,
        "far": (y + 2) % 4,
        "mate_d": x_lo * 2 + (1 - core),
        "side_d": (1 - x_lo) * 2 + core,
        "mate_side_d": (1 - x_lo) * 2 + (1 - core),
        "to_mate": {"depth": x_lo * 2 + (1 - core)},
        "to_side": {"depth": (1 - x_lo) * 2 + core},
        "to_up": {"narrow": (y + 1) % 4},
        "to_down": {"narrow": (y + 3) % 4},
    }


def scatter_sum(at, sems, base, part, own, mate_out, mate_in, ring_out, ring_in, side_out, side_in, finish):
    rows_all, quarter = own.shape[1:]
    rows, sub = rows_all // 4, quarter // 2
    pieces = [pl.ds(j * sub, sub) for j in range(2)]

    def bf16(value):
        return value.astype(jnp.bfloat16)

    def f32(value):
        return value.astype(jnp.float32)

    def rows_of(y):
        return pl.ds(pl.multiple_of(y * rows, rows), rows)

    def mate_copy(which, j):
        there = (which, slice(None), pieces[j])
        return remote(mate_out.at[there], mate_in.at[there], sems, base + which * 2 + j, at["to_mate"])

    def ring_copy(slot, j):
        there = (slot, slice(None), pieces[j])
        target = at["to_up"] if slot < 3 else at["to_down"]
        return remote(ring_out.at[there], ring_in.at[there], sems, base + 4 + slot * 2 + j, target)

    def side_copy(j):
        there = (slice(None), pieces[j])
        return remote(side_out.at[there], side_in.at[there], sems, base + 16 + j, at["to_side"])

    def produce(which, j):
        theirs, ours = ("mate_side_d", "side_d") if which else ("mate_d", "d")
        col = pl.multiple_of(at[theirs] * quarter + j * sub, sub)
        mate_out[which, :, pieces[j]] = bf16(part(col, sub))
        mate_copy(which, j).start()
        col = pl.multiple_of(at[ours] * quarter + j * sub, sub)
        own[which, :, pieces[j]] = part(col, sub)

    def pair(which, y, j):
        return own[which, rows_of(y), pieces[j]] + f32(mate_in[which, rows_of(y), pieces[j]])

    def got(slot, j):
        return f32(ring_in[slot, :, pieces[j]])

    def send(slot, j, value):
        ring_out[slot, :, pieces[j]] = bf16(value)
        ring_copy(slot, j).start()

    up, down, far, y = at["up"], at["down"], at["far"], at["y"]
    produce(1, 0)
    produce(1, 1)
    mate_copy(1, 0).wait_recv()
    send(3, 0, pair(1, far, 0))
    send(1, 0, pair(1, up, 0))
    produce(0, 0)
    mate_copy(1, 1).wait_recv()
    send(3, 1, pair(1, far, 1))
    send(1, 1, pair(1, up, 1))
    produce(0, 1)
    for j in range(2):
        mate_copy(0, j).wait_recv()
        send(0, j, pair(0, far, j))
    send(4, 0, pair(0, down, 0))
    for j in range(2):
        ring_copy(3, j).wait_recv()
        send(5, j, pair(1, down, j) + got(3, j))
    send(4, 1, pair(0, down, 1))
    for j in range(2):
        ring_copy(0, j).wait_recv()
        send(2, j, pair(0, up, j) + got(0, j))
    for j in range(2):
        ring_copy(1, j).wait_recv()
        ring_copy(5, j).wait_recv()
        side_out[:, pieces[j]] = bf16(pair(1, y, j) + got(1, j) + got(5, j))
        side_copy(j).start()
    for j in range(2):
        ring_copy(4, j).wait_recv()
        ring_copy(2, j).wait_recv()
        mine = pair(0, y, j) + got(4, j) + got(2, j)
        side_copy(j).wait_recv()
        finish(pieces[j], mine + f32(side_in[:, pieces[j]]))

    def wait_sent():
        for j in range(2):
            for which in range(2):
                mate_copy(which, j).wait_send()
            for slot in range(6):
                ring_copy(slot, j).wait_send()
            side_copy(j).wait_send()

    return wait_sent


def gather_all(at, sems, base, full, ready):
    rows, quarter = full.shape[0] // 4, full.shape[1] // 4
    sub = quarter // 2

    def block(y, d, piece):
        here = pl.ds(pl.multiple_of(y * rows, rows), rows)
        if piece is None:
            return full.at[here, pl.ds(pl.multiple_of(d * quarter, quarter), quarter)]
        return full.at[here, pl.ds(pl.multiple_of(d * quarter + piece * sub, sub), sub)]

    y, d, mate, side, mate_side = at["y"], at["d"], at["mate_d"], at["side_d"], at["mate_side_d"]
    up, down, far = at["up"], at["down"], at["far"]
    sent = []

    def send(slot, y, d, piece, target):
        ref = block(y, d, piece)
        copy = remote(ref, ref, sems, base + slot, at[target])
        copy.start()
        sent.append(copy)

    def arrived(slot, y, d, piece):
        ref = block(y, d, piece)
        remote(ref, ref, sems, base + slot, at["to_mate"]).wait_recv()

    send(0, y, d, 0, "to_side")
    send(2, y, d, 0, "to_up")
    send(4, y, d, 1, "to_down")
    send(1, y, d, 1, "to_side")
    send(3, y, d, 1, "to_up")
    send(5, y, d, 0, "to_down")
    send(6, y, d, None, "to_mate")
    arrived(0, y, side, 0)
    send(7, y, side, 0, "to_up")
    send(8, y, side, 0, "to_down")
    arrived(1, y, side, 1)
    send(9, y, side, 1, "to_down")
    send(10, y, side, 1, "to_up")
    send(11, y, side, None, "to_mate")
    arrived(2, down, d, 0)
    send(12, down, d, 0, "to_up")
    arrived(4, up, d, 1)
    send(13, up, d, 1, "to_down")
    arrived(3, down, d, 1)
    send(14, down, d, None, "to_mate")
    arrived(5, up, d, 0)
    send(15, up, d, None, "to_mate")
    arrived(6, y, mate, None)
    arrived(11, y, mate_side, None)
    ready(y)
    arrived(7, down, side, 0)
    send(16, down, side, 0, "to_up")
    arrived(9, up, side, 1)
    send(17, up, side, 1, "to_down")
    arrived(10, down, side, 1)
    send(18, down, side, None, "to_mate")
    arrived(8, up, side, 0)
    send(19, up, side, None, "to_mate")
    arrived(12, far, d, 0)
    arrived(13, far, d, 1)
    send(20, far, d, None, "to_mate")
    arrived(14, down, mate, None)
    arrived(18, down, mate_side, None)
    ready(down)
    arrived(16, far, side, 0)
    send(21, far, side, 0, "to_mate")
    arrived(17, far, side, 1)
    send(22, far, side, 1, "to_mate")
    arrived(15, up, mate, None)
    arrived(19, up, mate_side, None)
    ready(up)
    arrived(20, far, mate, None)
    arrived(21, far, mate_side, 0)
    arrived(22, far, mate_side, 1)
    ready(far)

    def wait_sent():
        for copy in sent:
            copy.wait_send()

    return wait_sent


def wide_places():
    w = lax.axis_index("wide")
    z, x = w // 2, w % 2
    up, down, far = (z + 1) % 4, (z + 3) % 4, (z + 2) % 4
    other = 1 - x
    order = [z * 2 + x, up * 2 + x, z * 2 + other, far * 2 + x, up * 2 + other, down * 2 + other, far * 2 + other, down * 2 + x]
    return {"w": w, "order": order}


OWN, UP, SIDE, FAR, UP_SIDE, DOWN_SIDE, FAR_SIDE, DOWN = range(8)
BACK = (OWN, DOWN, SIDE, FAR, DOWN_SIDE, UP_SIDE, FAR_SIDE, UP)


def attend(at, sems, base, set_up, asked, keys, values, marks, answer, returned, context):
    rows, feats = context.shape
    heads = feats // HEAD_DIM
    length = keys.shape[2]
    half = rows // 2
    order = at["order"]

    def send(slot, src_slot, dst_slot, target_slot, part=None):
        src, dst = asked.at[src_slot], asked.at[dst_slot]
        if part is not None:
            here = pl.ds(part * half, half)
            src, dst = asked.at[src_slot, here], asked.at[dst_slot, here]
        remote(src, dst, sems, base + slot, {"wide": order[target_slot]}).start()

    def arrived(slot, dst_slot, part=None):
        dst = asked.at[dst_slot] if part is None else asked.at[dst_slot, pl.ds(part * half, half)]
        remote(dst, dst, sems, base + slot, {"wide": order[SIDE]}).wait_recv()

    send(0, OWN, SIDE, SIDE)
    send(1, OWN, DOWN, UP)
    send(2, OWN, UP, DOWN)

    set_up()
    scale = HEAD_DIM ** (-0.5) * math.log2(math.e)

    def one_block(k, _):
        @pl.when(k == UP)
        def _():
            arrived(1, DOWN)
            send(3, DOWN, FAR, UP, 0)
            arrived(2, UP)
            send(4, UP, FAR, DOWN, 1)
            arrived(0, SIDE)
            send(5, SIDE, DOWN_SIDE, UP)
            send(6, SIDE, UP_SIDE, DOWN)

        @pl.when(k == FAR)
        def _():
            arrived(3, FAR, 0)
            arrived(4, FAR, 1)

        @pl.when(k == UP_SIDE)
        def _():
            arrived(5, DOWN_SIDE)
            send(7, DOWN_SIDE, FAR_SIDE, UP, 0)
            arrived(6, UP_SIDE)
            send(8, UP_SIDE, FAR_SIDE, DOWN, 1)

        @pl.when(k == FAR_SIDE)
        def _():
            arrived(7, FAR_SIDE, 0)
            arrived(8, FAR_SIDE, 1)

        source = jnp.int32(0)
        for slot in range(8):
            source = source + jnp.where(k == slot, order[slot], 0)
        lane = lax.broadcasted_iota(jnp.int32, marks.shape, 1)
        here = jnp.sum(jnp.where(lane == source, marks[...], 0.0), axis=1, keepdims=True)
        query = asked[k]
        total = jnp.zeros((rows, feats), jnp.float32)
        for head in range(heads):
            scores = jnp.dot(query, keys[head], preferred_element_type=jnp.float32)
            top = jnp.max(scores, axis=1, keepdims=True)
            weights = jnp.exp2((scores - top) * scale)
            below = jnp.sum(weights, axis=1, keepdims=True)
            taken = jnp.dot(weights.astype(jnp.bfloat16), values[head], preferred_element_type=jnp.float32)
            total = total + taken * (here / below)
        answer[k] = total.astype(jnp.bfloat16)
        for slot in range(1, 8):

            @pl.when(k == slot)
            def _():
                remote(
                    answer.at[slot], returned.at[BACK[slot]], sems, base + 8 + slot, {"wide": order[slot]}
                ).start()

        return 0

    lax.fori_loop(0, 8, one_block, 0)
    summed = answer[OWN].astype(jnp.float32)
    for slot in range(1, 8):
        remote(answer.at[slot], returned.at[BACK[slot]], sems, base + 8 + slot, {"wide": order[slot]}).wait_recv()
    for slot in range(1, 8):
        summed = summed + returned[slot].astype(jnp.float32)
    context[...] = summed.astype(jnp.bfloat16)

    def wait_sent():
        for slot in range(9):
            part = slot in (3, 4, 7, 8)
            src = asked.at[OWN, pl.ds(0, half)] if part else asked.at[OWN]
            remote(src, src, sems, base + slot, {"wide": order[SIDE]}).wait_send()
        for slot in range(1, 8):
            remote(answer.at[slot], returned.at[BACK[slot]], sems, base + 8 + slot, {"wide": order[slot]}).wait_send()

    return wait_sent


def spread_heads(kv, keys, values):
    heads = keys.shape[0]
    flipped = kv[0].T
    plain = kv[1]
    for head in range(heads):
        place = lax.broadcasted_iota(jnp.int32, flipped.shape, 0) // HEAD_DIM
        keys[head] = jnp.where(place == head, flipped, jnp.zeros_like(flipped))
        place = lax.broadcasted_iota(jnp.int32, plain.shape, 1) // HEAD_DIM
        values[head] = jnp.where(place == head, plain, jnp.zeros_like(plain))


def lay_out_small(router_rows, router_parts, expert_ids, pair_ids):
    exact = router_rows[...]
    high = exact.astype(jnp.bfloat16)
    middle = (exact - high.astype(jnp.float32)).astype(jnp.bfloat16)
    low = (exact - high.astype(jnp.float32) - middle.astype(jnp.float32)).astype(jnp.bfloat16)
    router_parts[...] = jnp.concatenate([high, middle, low, jnp.zeros_like(low)], axis=0)
    pad = jnp.zeros((6, expert_ids.shape[1]), jnp.float32)
    wide_ids = jnp.concatenate([expert_ids[...].astype(jnp.float32), pad], axis=0)
    pair_ids[...] = wide_ids.T.astype(jnp.int32)


def mark_rows(at, lang_ids, owner_slot, marks):
    rows = marks.shape[0]
    group = jnp.int32(0)
    for g in range(owner_slot.shape[0]):
        group = group + jnp.where(owner_slot[g] == at["w"], g, 0)
    spans = [lang_ids[:, block * rows : (block + 1) * rows] for block in range(8)]
    marks[...] = jnp.where(jnp.concatenate(spans, axis=0) == group, 1.0, 0.0).T


def layer_kernel(
    hidden_in_hbm,
    queries_hbm,
    lang_ids_hbm,
    owner_slot_hbm,
    enc_kv_hbm,
    attn_proj_hbm,
    norm_gain_hbm,
    router_rows_hbm,
    expert_ids_hbm,
    proj_in_hbm,
    proj_out_hbm,
    out,
    hidden_in,
    lang_ids,
    owner_slot,
    norm_gain,
    router_rows,
    expert_ids,
    asked,
    kv,
    keys,
    values,
    marks,
    answer,
    returned,
    context,
    attn_proj,
    proj_in,
    proj_out,
    full,
    normed,
    act,
    gate,
    router_parts,
    pair_ids,
    own,
    mate_out,
    mate_in,
    ring_out,
    ring_in,
    side_out,
    side_in,
    load_sems,
    send_sems,
    recv_sems,
):
    at, wide_at = places(), wide_places()
    sems = (send_sems, recv_sems)
    moves = [
        (queries_hbm, asked.at[OWN]),
        (enc_kv_hbm.at[0], kv),
        (lang_ids_hbm, lang_ids),
        (owner_slot_hbm, owner_slot),
        (attn_proj_hbm, attn_proj),
        (hidden_in_hbm, hidden_in),
        (norm_gain_hbm, norm_gain),
        (router_rows_hbm, router_rows),
        (expert_ids_hbm, expert_ids),
        (proj_in_hbm.at[0], proj_in),
        (proj_out_hbm.at[0], proj_out),
    ]
    loads = [pltpu.make_async_copy(src, dst, load_sems.at[i]) for i, (src, dst) in enumerate(moves)]
    loads[0].start()
    barrier = pltpu.get_barrier_semaphore()
    for slot in range(7, 0, -1):
        peer = {"wide": wide_at["order"][slot]}
        pl.semaphore_signal(barrier, inc=1, device_id=peer, device_id_type=MESH)
    for peer in ("to_mate", "to_side", "to_up", "to_down"):
        pl.semaphore_signal(barrier, inc=1, device_id=at[peer], device_id_type=MESH)
    for load in loads[1:]:
        load.start()
    loads[0].wait()
    pl.semaphore_wait(barrier, 11)

    def set_up():
        for i in (1, 2, 3):
            loads[i].wait()
        spread_heads(kv, keys, values)
        mark_rows(wide_at, lang_ids, owner_slot, marks)

    attend_sent = attend(
        wide_at, sems, 0, set_up, asked, keys, values, marks, answer, returned, context
    )
    for i in (4, 5, 6, 7, 8):
        loads[i].wait()

    rows, quarter = hidden_in.shape
    my_rows = pl.ds(pl.multiple_of(at["y"] * rows, rows), rows)

    def my_cols(piece):
        return pl.ds(pl.multiple_of(at["d"] * quarter + piece.start, piece.size), piece.size)

    def proj_part(col, size):
        return jnp.dot(
            context[...], attn_proj[:, pl.ds(col, size)], preferred_element_type=jnp.float32
        )

    def add_residual(piece, value):
        residual = hidden_in[:, piece].astype(jnp.float32) + value
        full[my_rows, my_cols(piece)] = residual.astype(jnp.bfloat16)

    proj_sent = scatter_sum(
        at, sems, 16, proj_part, own, mate_out.at[0], mate_in.at[0], ring_out.at[0], ring_in.at[0],
        side_out.at[0], side_in.at[0], add_residual,
    )
    lay_out_small(router_rows, router_parts, expert_ids, pair_ids)
    strip = 16

    def ready(y):
        def normalise(s, _):
            here = pl.ds(pl.multiple_of(y * rows + s * strip, strip), strip)
            value = full[here, :].astype(jnp.float32)
            inv = lax.rsqrt(jnp.mean(value * value, axis=1, keepdims=True) + norm_eps)
            normed[here, :] = (value * inv * norm_gain[...]).astype(jnp.bfloat16)
            return 0

        lax.fori_loop(0, rows // strip, normalise, 0)
        here = pl.ds(pl.multiple_of(y * rows, rows), rows)
        logit_parts = lax.dot_general(
            normed[here, :], router_parts[...], (((1,), (1,)), ((), ())), preferred_element_type=jnp.float32
        )
        first, second = pair_ids[here, 0:1], pair_ids[here, 1:2]
        chosen = (first == at["y"]) | (second == at["y"])
        other = first + second - at["y"]
        expert_of = lax.broadcasted_iota(jnp.int32, logit_parts.shape, 1) % 4
        signed = jnp.where(expert_of == at["y"], logit_parts, 0.0) - jnp.where(
            expert_of == other, logit_parts, 0.0
        )
        margin = jnp.sum(signed, axis=1, keepdims=True)
        gate[here, :] = jnp.where(chosen, 1.0 / (1.0 + jnp.exp(-margin)), 0.0)

    gather_sent = gather_all(at, sems, 34, full, ready)
    loads[9].wait()
    hidden = act.shape[1]
    step = 256 if hidden % 256 == 0 else hidden

    def first_layer(t, _):
        here = pl.ds(pl.multiple_of(t * step, step), step)
        value = jnp.dot(normed[...], proj_in[:, here], preferred_element_type=jnp.float32)
        act[:, here] = jax.nn.gelu(value, approximate=True).astype(jnp.bfloat16)
        return 0

    lax.fori_loop(0, hidden // step, first_layer, 0)
    loads[10].wait()

    def expert_part(col, size):
        return gate[...] * jnp.dot(
            act[...], proj_out[:, pl.ds(col, size)], preferred_element_type=jnp.float32
        )

    def add_experts(piece, value):
        residual = full[my_rows, my_cols(piece)].astype(jnp.float32)
        out[:, piece] = (residual + value).astype(jnp.bfloat16)

    expert_sent = scatter_sum(
        at, sems, 57, expert_part, own, mate_out.at[1], mate_in.at[1], ring_out.at[1], ring_in.at[1],
        side_out.at[1], side_in.at[1], add_experts,
    )
    for wait_sent in (attend_sent, proj_sent, gather_sent, expert_sent):
        wait_sent()


def layer_step(
    hidden_in,
    queries,
    lang_ids,
    owner_slot,
    enc_kv,
    attn_proj,
    norm_gain,
    router_proj,
    expert_ids,
    proj_in,
    proj_out,
):
    rows_all, inner = queries.shape
    rows, quarter = hidden_in.shape
    width = attn_proj.shape[1]
    hidden = proj_in.shape[2]
    length = enc_kv.shape[2]
    heads = inner // HEAD_DIM
    bf16, f32, i32 = jnp.bfloat16, jnp.float32, jnp.int32
    copies = 75
    return pl.pallas_call(
        layer_kernel,
        out_shape=pltpu.VMEM((rows, quarter), bf16),
        in_specs=[pl.BlockSpec(memory_space=pl.ANY)] * 11,
        out_specs=pl.BlockSpec(memory_space=pltpu.VMEM),
        scratch_shapes=[
            pltpu.VMEM((rows, quarter), bf16),
            pltpu.VMEM((1, lang_ids.shape[0]), i32),
            pltpu.SMEM(owner_slot.shape, i32),
            pltpu.VMEM((1, width), f32),
            pltpu.VMEM((4, width), f32),
            pltpu.VMEM((2, rows_all), i32),
            pltpu.VMEM((8, rows_all, inner), bf16),
            pltpu.VMEM((2, length, inner), bf16),
            pltpu.VMEM((heads, inner, length), bf16),
            pltpu.VMEM((heads, length, inner), bf16),
            pltpu.VMEM((rows_all, 8), f32),
            pltpu.VMEM((8, rows_all, inner), bf16),
            pltpu.VMEM((8, rows_all, inner), bf16),
            pltpu.VMEM((rows_all, inner), bf16),
            pltpu.VMEM((inner, width), bf16),
            pltpu.VMEM((width, hidden), bf16),
            pltpu.VMEM((hidden, width), bf16),
            pltpu.VMEM((rows_all, width), bf16),
            pltpu.VMEM((rows_all, width), bf16),
            pltpu.VMEM((rows_all, hidden), bf16),
            pltpu.VMEM((rows_all, 1), f32),
            pltpu.VMEM((16, width), bf16),
            pltpu.VMEM((rows_all, 8), i32),
            pltpu.VMEM((2, rows_all, quarter), f32),
            pltpu.VMEM((2, 2, rows_all, quarter), bf16),
            pltpu.VMEM((2, 2, rows_all, quarter), bf16),
            pltpu.VMEM((2, 6, rows, quarter), bf16),
            pltpu.VMEM((2, 6, rows, quarter), bf16),
            pltpu.VMEM((2, rows, quarter), bf16),
            pltpu.VMEM((2, rows, quarter), bf16),
            pltpu.SemaphoreType.DMA((11,)),
            pltpu.SemaphoreType.DMA((copies,)),
            pltpu.SemaphoreType.DMA((copies,)),
        ],
        compiler_params=pltpu.CompilerParams(
            collective_id=0, has_side_effects=True, vmem_limit_bytes=60 * 1024 * 1024
        ),
        name="layer_step",
    )(
        hidden_in,
        queries,
        lang_ids.reshape(1, -1),
        owner_slot,
        enc_kv,
        attn_proj,
        norm_gain.reshape(1, -1),
        router_proj.T,
        expert_ids.T,
        proj_in,
        proj_out,
    )


def solution(mesh):
    return jax.shard_map(
        layer_step,
        mesh=mesh,
        in_specs=(
            P(("wide", "narrow"), "depth"),
            P("wide", ("narrow", "depth")),
            P(),
            P(),
            P("wide", None, None, ("narrow", "depth")),
            P(("narrow", "depth"), None),
            P(),
            P(),
            P("wide", None),
            P("narrow", None, "depth"),
            P("narrow", "depth", None),
        ),
        out_specs=P(("wide", "narrow"), "depth"),
        check_vma=False,
    )
```
